16 devices in a mesh: data: 2 (over y, z), time: 8 (over x, core).
Axes of the slice: x: 4, y: 2, z: 1, core: 2. Of those that a mesh axis runs over, the one named last changes fastest.
The devices are a block of a 4x4x8 slice.
Arguments:
- x_init: float32 [16, 256, 16], P('data'), parts along dimension 0
- w_in: bfloat16 [16, 384], replicated
- w_out: bfloat16 [384, 16], replicated
- mod_scale: bfloat16 [32, 384], P('time')
- mod_shift: bfloat16 [32, 384], P('time')
- step_size: float32 [32], P('time')
- noise_inc: float32 [32, 16, 256, 16], P('time', 'data'), parts along dimension 1
Outputs:
- output: float32 [32, 16, 256, 16], P('time', 'data'), parts along dimension 1
There are 2 independent parts. The reference program is written for one: setup_inputs(seed, part) draws one part's arguments, and reference() takes and returns one part's arrays. A program takes and returns all parts, laid end to end along the dimension named above; an argument that names none is the same for every part.
All inputs are finite; a program needn't handle non-finite values.
Results may differ from the reference program's by a relative error of at most 0.001.
Values are sent between devices in bfloat16 or wider.
A program may use at most 768 MiB of HBM per device.

```python
import jax
import jax.numpy as jnp
from jax import lax

BATCH = 8
TOKENS = 256
CHANNELS = 16
HIDDEN = 384
STEPS = 32
SWEEPS = 8


def setup_inputs(seed: int = 0, part: int = 0) -> dict:
    base_key = jax.random.key(seed)
    part_key = jax.random.fold_in(base_key, part)
    key_lat, key_noise = jax.random.split(part_key, 2)
    key_list = jax.random.split(jax.random.key(seed + 1), 6)
    w_first = jax.random.normal(key_list[0], (CHANNELS, HIDDEN), jnp.float32) * CHANNELS ** -0.5
    w_back = -(2.0 * CHANNELS / HIDDEN) * w_first.T + 0.5 * HIDDEN ** -0.5 * jax.random.normal(key_list[1], (HIDDEN, CHANNELS), jnp.float32)
    mod_scale = 0.2 * jax.random.normal(key_list[2], (STEPS, HIDDEN), jnp.float32)
    mod_shift = 0.5 * jax.random.normal(key_list[3], (STEPS, HIDDEN), jnp.float32)
    position = (jnp.arange(STEPS, dtype=jnp.float32) + 0.5) / STEPS
    tilt_coef = jax.random.uniform(key_list[4], (), jnp.float32, -1.0, 1.0)
    jitter = jax.random.uniform(key_list[5], (STEPS,), jnp.float32, 0.75, 1.25)
    step_size = (3.0 / STEPS) * jnp.exp(tilt_coef * (position - 0.5)) * jitter
    x_init = jax.random.normal(key_lat, (BATCH, TOKENS, CHANNELS), jnp.float32)
    noise_inc = 2.0 * STEPS ** -0.5 * jax.random.normal(key_noise, (STEPS, BATCH, TOKENS, CHANNELS), jnp.float32)
    return {
        "x_init": x_init,
        "w_in": w_first.astype(jnp.bfloat16),
        "w_out": w_back.astype(jnp.bfloat16),
        "mod_scale": mod_scale.astype(jnp.bfloat16),
        "mod_shift": mod_shift.astype(jnp.bfloat16),
        "step_size": step_size,
        "noise_inc": noise_inc,
    }


def drift_one(latents, scale_row, shift_row, step_row, w_in, w_out):
    flat_lat = latents.astype(jnp.bfloat16).reshape(BATCH * TOKENS, CHANNELS)
    pre_act = jnp.dot(flat_lat, w_in, preferred_element_type=jnp.float32)
    hidden = pre_act * (1.0 + scale_row.astype(jnp.float32)) + shift_row.astype(jnp.float32)
    gelu_out = jax.nn.gelu(hidden, approximate=True).astype(jnp.bfloat16)
    proj_out = jnp.dot(gelu_out, w_out, preferred_element_type=jnp.float32)
    return (step_row * proj_out).reshape(BATCH, TOKENS, CHANNELS)


def reference(x_init, w_in, w_out, mod_scale, mod_shift, step_size, noise_inc):
    def one_sweep(latents, unused):
        drifts = lax.map(lambda fields: drift_one(fields[0], fields[1], fields[2], fields[3], w_in, w_out), (latents, mod_scale, mod_shift, step_size))
        increments = drifts + noise_inc
        earlier = jnp.concatenate([jnp.zeros_like(increments[:1]), jnp.cumsum(increments[:-1], axis=0)], axis=0)
        return x_init[None] + earlier, None
    start_lat = jnp.broadcast_to(x_init[None], noise_inc.shape)
    final_lat, unused = lax.scan(one_sweep, start_lat, None, length=SWEEPS)
    return final_lat
```

```python
import functools
import math

import jax
import jax.numpy as jnp
from jax import lax
from jax.experimental import pallas as pl
from jax.experimental.pallas import tpu as pltpu
from jax.sharding import PartitionSpec as P

SWEEPS = 8
LANES = 128
F32 = jnp.float32
BF16 = jnp.bfloat16
MESH = pl.DeviceIdType.MESH
GELU_1 = 2.0 * math.sqrt(2.0 / math.pi)
GELU_3 = 4.0 * 0.044715 * GELU_1
CONST_ROW = 64


def gelu_of_half(half):
    inner = half * (half * half * GELU_3 + GELU_1)
    return half + half * jnp.tanh(inner)


def sampler_kernel(n_time, x_ref, w_in_ref, w_out_ref, scale_ref, shift_ref, step_ref, noise_ref, out_ref,
                   x_buf, w_in_t, mod_own, step_own, mod_all, step_all, mod_t, mul_buf, add_buf, pre_init,
                   versions, act_buf, act_late, noise_all, out_stage,
                   x_sem, mod_send, mod_recv, step_send, step_recv, noise_send, noise_recv, out_send, out_recv):
    me = lax.axis_index("time")
    local_steps = scale_ref.shape[0]
    n_steps = n_time * local_steps
    hidden = w_in_ref.shape[1]
    tokens = x_buf.shape[1]
    copies = tokens // LANES

    barrier = pltpu.get_barrier_semaphore()
    for away in range(1, n_time):
        pl.semaphore_signal(barrier, inc=1, device_id={"time": lax.rem(me + away, n_time)}, device_id_type=MESH)

    x_copy = pltpu.make_async_copy(x_ref.at[me], x_buf, x_sem)
    x_copy.start()
    own_noise = pltpu.make_async_copy(noise_ref.at[:, me], noise_all.at[pl.ds(me * local_steps, local_steps)], noise_recv.at[me])
    own_noise.start()
    mod_own[0:local_steps, :] = scale_ref[...]
    mod_own[local_steps:2 * local_steps, :] = shift_ref[...]
    for i in range(local_steps):
        step_own[i:i + 1, :] = jnp.full((1, LANES), step_ref[i], F32)
    mod_all[me] = mod_own[...]
    step_all[me] = step_own[...]
    w_in_t[...] = w_in_ref[...].astype(F32).T.astype(BF16)

    pl.semaphore_wait(barrier, n_time - 1)

    sends = []

    def send(src, dst, send_sem, recv_sem, target):
        copy = pltpu.make_async_remote_copy(src_ref=src, dst_ref=dst, send_sem=send_sem, recv_sem=recv_sem,
                                            device_id={"time": target}, device_id_type=MESH)
        copy.start()
        return copy

    for away in range(1, n_time):
        target = lax.rem(me + away, n_time)
        sends.append(send(mod_own, mod_all.at[me], mod_send.at[away], mod_recv.at[away], target))
        sends.append(send(step_own, step_all.at[me], step_send.at[away], step_recv.at[away], target))
    for away in range(1, n_time):
        target = lax.rem(me + away, n_time)
        sends.append(send(noise_ref.at[:, target], noise_all.at[pl.ds(me * local_steps, local_steps)],
                          noise_send.at[away], noise_recv.at[me], target))

    x_copy.wait()
    x0 = x_buf[...]
    for s in range(SWEEPS + 1):
        versions[s] = x0
    pre_init[...] = jnp.dot(w_in_t[...], x0.astype(BF16), preferred_element_type=F32)

    for away in range(1, n_time):
        source = lax.rem(me + n_time - away, n_time)
        pltpu.make_async_copy(mod_own, mod_all.at[source], mod_recv.at[away]).wait()
        pltpu.make_async_copy(step_own, step_all.at[source], step_recv.at[away]).wait()

    rows = mod_all[...].astype(F32).reshape(n_time * 2 * local_steps, hidden)
    pad = (lax.broadcasted_iota(jnp.int32, (LANES - CONST_ROW, hidden), 0) == 0).astype(F32)
    mod_t[...] = jnp.concatenate([rows, pad], axis=0).T.astype(BF16)

    def column_of(block, i):
        block = block + i // local_steps
        return block * 2 * local_steps + i % local_steps

    def prepare(block, steps):
        row = lax.broadcasted_iota(jnp.int32, (LANES, LANES), 0)
        picks = []
        for i in steps:
            at = column_of(block, i)
            picks.append(jnp.where((row == at) | (row == CONST_ROW), 0.5, 0.0).astype(BF16))
            picks.append(jnp.where(row == at + local_steps, 0.5, 0.0).astype(BF16))
        both = jnp.dot(mod_t[...], jnp.concatenate(picks, axis=1), preferred_element_type=F32)
        for k, i in enumerate(steps):
            mul_buf[i % local_steps] = both[:, 2 * k * LANES:(2 * k + 1) * LANES]
            add_buf[i % local_steps] = both[:, (2 * k + 1) * LANES:(2 * k + 2) * LANES]

    def wide(row):
        return jnp.concatenate([row] * copies, axis=1)

    def activate(pre, slot, dst, index):
        half = pre * wide(mul_buf[slot]) + wide(add_buf[slot])
        dst[index] = gelu_of_half(half).astype(BF16)

    def first_product(s):
        return jnp.dot(w_in_t[...], versions[s].astype(BF16), preferred_element_type=F32)

    def update(block, i, s, act, base=None):
        at = block * local_steps + i
        drift = jnp.dot(w_out_ref[...], act, preferred_element_type=F32)
        step = wide(step_all[block + i // local_steps, pl.ds(i % local_steps, 1), :])
        versions[s + 1] = versions[s + 1 if base is None else base] + (drift * step + noise_all[at])

    def run_block(block, first, last, static_block=None, late=None, keep_late=True):
        for i in range(first, last):
            if static_block is None:
                low, high = 0, SWEEPS - 1
            else:
                j = static_block * local_steps + i
                low, high = max(0, SWEEPS - (n_steps - 1 - j)), min(j, SWEEPS - 1)
            slot = i % local_steps
            out_stage[block * local_steps + i] = versions[min(high + 1, SWEEPS) if static_block is None or j >= SWEEPS else j]
            if low > high:
                continue
            if i % 2 == 0:
                steps = (i + 1, i + 2)
                if static_block is not None:
                    steps = tuple(k for k in steps if static_block * local_steps + k < n_steps - 1)
                if steps:
                    prepare(block, steps)
            if late is not None:
                update(*late, act_late[...])
                late = None
            order = ([0] if low == 0 else []) + list(range(high, max(low, 1) - 1, -1))
            pre = pre_init[...] if order[0] == 0 else first_product(order[0])
            waiting = []
            for k, s in enumerate(order):
                following = first_product(order[k + 1]) if k + 1 < len(order) else None
                is_late = keep_late and i == last - 1 and k == len(order) - 1 and s != 0
                if is_late:
                    activate(pre, slot, act_late, ...)
                    late = (block, i, s)
                else:
                    activate(pre, slot, act_buf, (i % 2) * SWEEPS + s)
                pre = following
                waiting.append(s)
                ready = [w for w in waiting[:-1] if w != 0]
                for w in ready:
                    fresh = static_block is not None and w == j
                    update(block, i, w, act_buf[(i % 2) * SWEEPS + w], w if fresh else None)
                    waiting.remove(w)
            for w in sorted(waiting, reverse=True):
                if late is not None and w == late[2]:
                    continue
                fresh = static_block is not None and w == j
                update(block, i, w, act_buf[(i % 2) * SWEEPS + w], w if fresh else None)
        return late

    def wait_noise(block):
        dst = noise_all.at[pl.ds(block * local_steps, local_steps)]
        pltpu.make_async_copy(noise_ref.at[:, me], dst, noise_recv.at[block]).wait()

    def send_block(block):
        src = out_stage.at[pl.ds(block * local_steps, local_steps)]

        @pl.when(block != me)
        def _():
            send(src, out_ref.at[:, me], out_send.at[block], out_recv.at[me], block)

        @pl.when(block == me)
        def _():
            out_ref[:, me] = src[...]

    full_from = -(-(SWEEPS - 1) // local_steps)
    full_to = (n_steps - SWEEPS) // local_steps

    prepare(0, (0,))
    late = None
    for block in range(full_from):
        wait_noise(block)
        late = run_block(block, 0, local_steps, block, late)
        if block > 0:
            send_block(block - 1)

    def body(block, carry):
        wait_noise(block)
        send_block(block - 1)
        run_block(block, 0, local_steps, None, (block - 1, local_steps - 1, 1))
        return carry

    lax.fori_loop(full_from, full_to, body, 0)
    late = (full_to - 1, local_steps - 1, 1)
    for block in range(full_to, n_time):
        wait_noise(block)
        send_block(block - 1)
        late = run_block(block, 0, local_steps, block, late, keep_late=block < n_time - 1)
    send_block(n_time - 1)

    for copy in sends:
        copy.wait_send()
    for away in range(1, n_time):
        other = lax.rem(me + away, n_time)
        done = pltpu.make_async_remote_copy(src_ref=out_stage.at[pl.ds(other * local_steps, local_steps)], dst_ref=out_ref.at[:, other],
                                            send_sem=out_send.at[other], recv_sem=out_recv.at[other],
                                            device_id={"time": other}, device_id_type=MESH)
        done.wait_send()
        done.wait_recv()


def solution(mesh):
    n_time = mesh.shape["time"]

    def body(x_init, w_in, w_out, mod_scale, mod_shift, step_size, noise_inc):
        local_steps, batch, tokens, channels = noise_inc.shape
        hidden = w_in.shape[1]
        assert batch == n_time and 2 * local_steps * n_time == CONST_ROW
        x_t = jnp.swapaxes(x_init, 1, 2)
        noise_t = jnp.swapaxes(noise_inc, 2, 3)
        n_steps = n_time * local_steps
        vmem = pl.BlockSpec(memory_space=pltpu.VMEM)
        anywhere = pl.BlockSpec(memory_space=pl.ANY)
        dma = pltpu.SemaphoreType.DMA
        out = pl.pallas_call(
            functools.partial(sampler_kernel, n_time),
            out_shape=jax.ShapeDtypeStruct(noise_t.shape, F32),
            in_specs=[anywhere, vmem, vmem, vmem, vmem, pl.BlockSpec(memory_space=pltpu.SMEM), anywhere],
            out_specs=vmem,
            scratch_shapes=[
                pltpu.VMEM((channels, tokens), F32),
                pltpu.VMEM((hidden, channels), BF16),
                pltpu.VMEM((2 * local_steps, hidden), BF16),
                pltpu.VMEM((2 * local_steps, LANES), F32),
                pltpu.VMEM((n_time, 2 * local_steps, hidden), BF16),
                pltpu.VMEM((n_time, 2 * local_steps, LANES), F32),
                pltpu.VMEM((hidden, LANES), BF16),
                pltpu.VMEM((local_steps, hidden, LANES), F32),
                pltpu.VMEM((local_steps, hidden, LANES), F32),
                pltpu.VMEM((hidden, tokens), F32),
                pltpu.VMEM((SWEEPS + 1, channels, tokens), F32),
                pltpu.VMEM((2 * SWEEPS, hidden, tokens), BF16),
                pltpu.VMEM((hidden, tokens), BF16),
                pltpu.VMEM((n_steps, channels, tokens), F32),
                pltpu.VMEM((n_steps, channels, tokens), F32),
                dma, dma((n_time,)), dma((n_time,)), dma((n_time,)), dma((n_time,)),
                dma((n_time,)), dma((n_time,)), dma((n_time,)), dma((n_time,)),
            ],
            compiler_params=pltpu.CompilerParams(collective_id=0, has_side_effects=True),
        )(x_t, w_in, w_out.T, mod_scale, mod_shift, step_size, noise_t)
        return jnp.swapaxes(out, 2, 3)

    return jax.shard_map(
        body,
        mesh=mesh,
        in_specs=(P("data"), P(), P(), P("time"), P("time"), P("time"), P("time", "data")),
        out_specs=P("time", "data"),
        check_vma=False,
    )
```

```python
import functools
import math

import jax
import jax.numpy as jnp
from jax import lax
from jax.experimental import pallas as pl
from jax.experimental.pallas import tpu as pltpu
from jax.sharding import PartitionSpec as P

SWEEPS = 8
LANES = 128
F32 = jnp.float32
BF16 = jnp.bfloat16
MESH = pl.DeviceIdType.MESH
GELU_1 = 2.0 * math.sqrt(2.0 / math.pi)
GELU_3 = 4.0 * 0.044715 * GELU_1
CONST_ROW = 64


def gelu_of_half(half):
    inner = half * (half * half * GELU_3 + GELU_1)
    return half + half * jnp.tanh(inner)


def sampler_kernel(n_time, x_ref, w_in_ref, w_out_ref, scale_ref, shift_ref, step_ref, noise_ref, out_ref,
                   x_buf, w_in_buf, w_out_buf, scale_buf, shift_buf, step_buf,
                   w_in_t, mod_own, step_own, mod_all, step_all, mod_t, mul_buf, add_buf, pre_init,
                   versions, act_buf, act_late, noise_all, out_stage, gathered,
                   load_sem, mod_send, mod_recv, step_send, step_recv, noise_send, noise_recv, out_send, out_recv):
    me = lax.axis_index("time")
    local_steps = scale_ref.shape[0]
    partner = me + 1 - 2 * lax.rem(me, 2)
    n_steps = n_time * local_steps
    hidden = w_in_ref.shape[1]
    tokens = x_buf.shape[1]
    copies = tokens // LANES

    barrier = pltpu.get_barrier_semaphore()
    for away in range(1, n_time):
        pl.semaphore_signal(barrier, inc=1, device_id={"time": lax.rem(me + away, n_time)}, device_id_type=MESH)

    loads = [
        pltpu.make_async_copy(src, dst, load_sem.at[k])
        for k, (src, dst) in enumerate([(scale_ref, scale_buf), (shift_ref, shift_buf), (step_ref, step_buf),
                                        (w_in_ref, w_in_buf), (x_ref.at[me], x_buf), (w_out_ref, w_out_buf)])
    ]
    for copy in loads:
        copy.start()
    own_noise = pltpu.make_async_copy(noise_ref.at[:, me], noise_all.at[pl.ds(me * local_steps, local_steps)], noise_recv.at[me])
    own_noise.start()
    for copy in loads:
        copy.wait()
    mod_own[0:local_steps, :] = scale_buf[...]
    mod_own[local_steps:2 * local_steps, :] = shift_buf[...]
    for i in range(local_steps):
        step_own[i:i + 1, :] = jnp.full((1, LANES), step_buf[i], F32)
    mod_all[me] = mod_own[...]
    step_all[me] = step_own[...]
    w_in_t[...] = w_in_buf[...].astype(F32).T.astype(BF16)

    x0 = x_buf[...]
    for s in range(SWEEPS + 1):
        versions[s] = x0
    out_stage[0] = x0
    pre_init[...] = jnp.dot(w_in_t[...], x0.astype(BF16), preferred_element_type=F32)

    pl.semaphore_wait(barrier, n_time - 1)

    sends = []

    def send(src, dst, send_sem, recv_sem, target):
        copy = pltpu.make_async_remote_copy(src_ref=src, dst_ref=dst, send_sem=send_sem, recv_sem=recv_sem,
                                            device_id={"time": target}, device_id_type=MESH)
        copy.start()
        return copy

    for away in range(1, n_time):
        target = lax.rem(me + away, n_time)
        sends.append(send(mod_own, mod_all.at[me], mod_send.at[away], mod_recv.at[away], target))
        sends.append(send(step_own, step_all.at[me], step_send.at[away], step_recv.at[away], target))
    for away in range(1, n_time):
        target = lax.rem(me + away, n_time)
        sends.append(send(noise_ref.at[:, target], noise_all.at[pl.ds(me * local_steps, local_steps)],
                          noise_send.at[away], noise_recv.at[me], target))

    for away in range(1, n_time):
        source = lax.rem(me + n_time - away, n_time)
        pltpu.make_async_copy(mod_own, mod_all.at[source], mod_recv.at[away]).wait()
        pltpu.make_async_copy(step_own, step_all.at[source], step_recv.at[away]).wait()

    rows = mod_all[...].astype(F32).reshape(n_time * 2 * local_steps, hidden)
    pad = (lax.broadcasted_iota(jnp.int32, (LANES - CONST_ROW, hidden), 0) == 0).astype(F32)
    mod_t[...] = jnp.concatenate([rows, pad], axis=0).T.astype(BF16)

    def column_of(block, i):
        block = block + i // local_steps
        return block * 2 * local_steps + i % local_steps

    def prepare(block, steps):
        row = lax.broadcasted_iota(jnp.int32, (LANES, LANES), 0)
        picks = []
        for i in steps:
            at = column_of(block, i)
            picks.append(jnp.where((row == at) | (row == CONST_ROW), 0.5, 0.0).astype(BF16))
            picks.append(jnp.where(row == at + local_steps, 0.5, 0.0).astype(BF16))
        both = jnp.dot(mod_t[...], jnp.concatenate(picks, axis=1), preferred_element_type=F32)
        for k, i in enumerate(steps):
            mul_buf[i % local_steps] = both[:, 2 * k * LANES:(2 * k + 1) * LANES]
            add_buf[i % local_steps] = both[:, (2 * k + 1) * LANES:(2 * k + 2) * LANES]

    def wide(row):
        return jnp.concatenate([row] * copies, axis=1)

    def activate(pre, slot, dst, index):
        half = pre * wide(mul_buf[slot]) + wide(add_buf[slot])
        dst[index] = gelu_of_half(half)

    def first_product(s):
        return jnp.dot(w_in_t[...], versions[s].astype(BF16), preferred_element_type=F32)

    def update(block, i, s, act, base=None):
        at = block * local_steps + i
        done = s == SWEEPS - 1 or base is not None
        drift = jnp.dot(w_out_buf[...], act.astype(BF16), preferred_element_type=F32)
        step = wide(step_all[block + i // local_steps, pl.ds(i % local_steps, 1), :])
        versions[s + 1] = versions[s + 1 if base is None else base] + (drift * step + noise_all[at])
        if done:
            out_stage[at + 1] = versions[s + 1]
            if isinstance(block, int):
                send_ready(block, i + 1)

    def run_block(block, first, last, static_block=None, late=None, keep_late=True):
        for i in range(first, last):
            if static_block is None:
                low, high = 0, SWEEPS - 1
            else:
                j = static_block * local_steps + i
                low, high = max(0, SWEEPS - (n_steps - 1 - j)), min(j, SWEEPS - 1)
            slot = i % local_steps
            if low > high:
                continue
            if i % 2 == 0:
                steps = (i + 1, i + 2)
                if static_block is not None:
                    steps = tuple(k for k in steps if static_block * local_steps + k < n_steps - 1)
                if steps:
                    prepare(block, steps)
            if late is not None:
                update(*late, act_late[...])
                late = None
            order = ([0] if low == 0 else []) + list(range(high, max(low, 1) - 1, -1))
            pre = pre_init[...] if order[0] == 0 else first_product(order[0])
            waiting = []
            for k, s in enumerate(order):
                following = first_product(order[k + 1]) if k + 1 < len(order) else None
                is_late = keep_late and i == last - 1 and k == len(order) - 1 and s != 0
                if is_late:
                    activate(pre, slot, act_late, ...)
                    late = (block, i, s)
                else:
                    activate(pre, slot, act_buf, (i % 2) * SWEEPS + s)
                pre = following
                waiting.append(s)
                ready = [w for w in waiting[:-1] if w != 0]
                for w in ready:
                    fresh = static_block is not None and w == j
                    update(block, i, w, act_buf[(i % 2) * SWEEPS + w], w if fresh else None)
                    waiting.remove(w)
            for w in sorted(waiting, reverse=True):
                if late is not None and w == late[2]:
                    continue
                fresh = static_block is not None and w == j
                update(block, i, w, act_buf[(i % 2) * SWEEPS + w], w if fresh else None)
        return late

    def wait_noise(block):
        dst = noise_all.at[pl.ds(block * local_steps, local_steps)]
        pltpu.make_async_copy(noise_ref.at[:, me], dst, noise_recv.at[block]).wait()

    def send_steps(block, first, count):
        own = block == me
        send(out_stage.at[pl.ds(block * local_steps + first, count)],
             gathered.at[pl.ds(first, count), jnp.where(own, n_time, me)],
             out_send.at[block], out_recv.at[jnp.where(own, n_time, me)], jnp.where(own, partner, block))

    def send_ready(block, i):
        block, i = block + i // local_steps, i % local_steps
        if block == n_time - 2 and i >= local_steps - 2:
            if i == local_steps - 2:
                send_steps(block, 0, i + 1)
            else:
                send_steps(block, i, 1)
        if block == n_time - 1:
            send_steps(block, i, 1)

    full_from = -(-(SWEEPS - 1) // local_steps)
    full_to = (n_steps - SWEEPS) // local_steps

    prepare(0, (0,))
    late = None
    for block in range(full_from):
        wait_noise(block)
        late = run_block(block, 0, local_steps, block, late)
        if block > 0:
            send_steps(block - 1, 0, local_steps)

    def body(block, carry):
        wait_noise(block)
        send_steps(block - 1, 0, local_steps)
        run_block(block, 0, local_steps, None, (block - 1, local_steps - 1, 1))
        return carry

    lax.fori_loop(full_from, full_to, body, 0)
    late = (full_to - 1, local_steps - 1, 1)
    for block in range(full_to, n_time):
        wait_noise(block)
        if block == full_to:
            send_steps(block - 1, 0, local_steps)
        late = run_block(block, 0, local_steps, block, late, keep_late=block < n_time - 1)

    for copy in sends:
        copy.wait_send()
    for away in range(n_time):
        other = lax.rem(me + away, n_time)
        slot = n_time if away == 0 else other
        done = pltpu.make_async_remote_copy(src_ref=out_stage.at[pl.ds(other * local_steps, local_steps)], dst_ref=gathered.at[:, slot],
                                            send_sem=out_send.at[other], recv_sem=out_recv.at[slot],
                                            device_id={"time": partner}, device_id_type=MESH)
        done.wait_send()
        done.wait_recv()
        if away == 0:
            out_ref[:, me] = out_stage[pl.ds(me * local_steps, local_steps)]
        else:
            out_ref[:, other] = gathered[:, other]


def solution(mesh):
    n_time = mesh.shape["time"]

    def body(x_init, w_in, w_out, mod_scale, mod_shift, step_size, noise_inc):
        local_steps, batch, tokens, channels = noise_inc.shape
        hidden = w_in.shape[1]
        assert batch == n_time and 2 * local_steps * n_time == CONST_ROW
        x_t = jnp.swapaxes(x_init, 1, 2)
        noise_t = jnp.swapaxes(noise_inc, 2, 3)
        n_steps = n_time * local_steps
        vmem = pl.BlockSpec(memory_space=pltpu.VMEM)
        anywhere = pl.BlockSpec(memory_space=pl.ANY)
        dma = pltpu.SemaphoreType.DMA
        out = pl.pallas_call(
            functools.partial(sampler_kernel, n_time),
            out_shape=pltpu.VMEM(noise_t.shape, F32),
            in_specs=[anywhere] * 7,
            out_specs=vmem,
            scratch_shapes=[
                pltpu.VMEM((channels, tokens), F32),
                pltpu.VMEM((channels, hidden), BF16),
                pltpu.VMEM((channels, hidden), BF16),
                pltpu.VMEM((local_steps, hidden), BF16),
                pltpu.VMEM((local_steps, hidden), BF16),
                pltpu.SMEM((local_steps,), F32),
                pltpu.VMEM((hidden, channels), BF16),
                pltpu.VMEM((2 * local_steps, hidden), BF16),
                pltpu.VMEM((2 * local_steps, LANES), F32),
                pltpu.VMEM((n_time, 2 * local_steps, hidden), BF16),
                pltpu.VMEM((n_time, 2 * local_steps, LANES), F32),
                pltpu.VMEM((hidden, LANES), BF16),
                pltpu.VMEM((local_steps, hidden, LANES), F32),
                pltpu.VMEM((local_steps, hidden, LANES), F32),
                pltpu.VMEM((hidden, tokens), F32),
                pltpu.VMEM((SWEEPS + 1, channels, tokens), F32),
                pltpu.VMEM((2 * SWEEPS, hidden, tokens), F32),
                pltpu.VMEM((hidden, tokens), F32),
                pltpu.VMEM((n_steps, channels, tokens), F32),
                pltpu.VMEM((n_steps, channels, tokens), F32),
                pltpu.VMEM((local_steps, n_time + 1, channels, tokens), F32),
                dma((6,)), dma((n_time,)), dma((n_time,)), dma((n_time,)), dma((n_time,)),
                dma((n_time,)), dma((n_time,)), dma((n_time,)), dma((n_time + 1,)),
            ],
            compiler_params=pltpu.CompilerParams(collective_id=0, has_side_effects=True),
        )(x_t, w_in, w_out.T, mod_scale, mod_shift, step_size, noise_t)
        return jnp.swapaxes(out, 2, 3)

    return jax.shard_map(
        body,
        mesh=mesh,
        in_specs=(P("data"), P(), P(), P("time"), P("time"), P("time"), P("time", "data")),
        out_specs=P("time", "data"),
        check_vma=False,
    )
```

```python
import functools
import math

import jax
import jax.numpy as jnp
from jax import lax
from jax.experimental import pallas as pl
from jax.experimental.pallas import tpu as pltpu
from jax.sharding import PartitionSpec as P

SWEEPS = 8
UPWARD = 6
LANES = 128
F32 = jnp.float32
BF16 = jnp.bfloat16
MESH = pl.DeviceIdType.MESH
GELU_1 = 2.0 * math.sqrt(2.0 / math.pi)
GELU_3 = 4.0 * 0.044715 * GELU_1


def gelu_of_half(half):
    inner = half * (half * half * GELU_3 + GELU_1)
    return half + half * jnp.tanh(inner)


def sampler_kernel(n_time, x_ref, w_in_ref, w_out_ref, scale_ref, shift_ref, step_ref, noise_ref, out_ref,
                   x_buf, w_in_buf, w_out_buf, scale_buf, shift_buf, step_buf, noise_buf,
                   w_in_t, mod_own, step_own, mod_all, step_all, mul_all, add_all, pre_init, first_drift,
                   versions, act_buf, act_late, pre_late, act_init, noise_all, out_stage, gathered,
                   load_sem, mod_send, mod_recv, step_send, step_recv, noise_send, noise_recv, out_send, out_recv):
    me = lax.axis_index("time")
    local_steps = scale_ref.shape[0]
    partner = me + 1 - 2 * lax.rem(me, 2)
    n_steps = n_time * local_steps
    hidden = w_in_ref.shape[1]
    tokens = x_buf.shape[1]
    copies = tokens // LANES

    barrier = pltpu.get_barrier_semaphore()
    for away in range(1, n_time):
        pl.semaphore_signal(barrier, inc=1, device_id={"time": lax.rem(me + away, n_time)}, device_id_type=MESH)

    loads = [
        pltpu.make_async_copy(src, dst, load_sem.at[k])
        for k, (src, dst) in enumerate([(scale_ref, scale_buf), (shift_ref, shift_buf), (step_ref, step_buf),
                                        (w_in_ref, w_in_buf), (x_ref.at[me], x_buf), (w_out_ref, w_out_buf)])
    ]
    for copy in loads:
        copy.start()
    own_noise = pltpu.make_async_copy(noise_ref.at[:, me], noise_all.at[pl.ds(me * local_steps, local_steps)], noise_recv.at[me])
    own_noise.start()
    noise_load = pltpu.make_async_copy(noise_ref, noise_buf, load_sem.at[len(loads)])
    noise_load.start()
    for copy in loads:
        copy.wait()
    mod_own[0:local_steps, :] = scale_buf[...]
    mod_own[local_steps:2 * local_steps, :] = shift_buf[...]
    for i in range(local_steps):
        step_own[i:i + 1, :] = jnp.full((1, LANES), step_buf[i], F32)
    mod_all[me] = mod_own[...]
    step_all[me] = step_own[...]
    w_in_t[...] = w_in_buf[...].astype(F32).T.astype(BF16)

    x0 = x_buf[...]
    versions[0, 0] = x0
    versions[1, 0] = x0
    out_stage[0] = x0
    pre_init[...] = jnp.dot(w_in_t[...], x0.astype(BF16), preferred_element_type=F32)

    pl.semaphore_wait(barrier, n_time - 1)

    sends = []

    def send(src, dst, send_sem, recv_sem, target):
        copy = pltpu.make_async_remote_copy(src_ref=src, dst_ref=dst, send_sem=send_sem, recv_sem=recv_sem,
                                            device_id={"time": target}, device_id_type=MESH)
        copy.start()
        return copy

    n_chips = n_time // 2
    chip, core = me // 2, lax.rem(me, 2)
    apart = sorted(range(1, n_chips), key=lambda hops: -min(hops, n_chips - hops))
    peers = [2 * lax.rem(chip + hops, n_chips) + c for hops in apart for c in range(2)] + [partner]
    for k, target in enumerate(peers):
        sends.append(send(mod_own, mod_all.at[me], mod_send.at[k], mod_recv.at[me], target))
        sends.append(send(step_own, step_all.at[me], step_send.at[k], step_recv.at[me], target))
    noise_load.wait()

    def noise_copy(k):
        return pltpu.make_async_remote_copy(
            src_ref=noise_buf.at[:, peers[k]], dst_ref=noise_all.at[pl.ds(me * local_steps, local_steps)],
            send_sem=noise_send.at[k], recv_sem=noise_recv.at[me], device_id={"time": peers[k]}, device_id_type=MESH)

    def send_noise():
        for k in range(n_time - 1):
            noise_copy(k).start()

    def wait_mods(source):
        pltpu.make_async_copy(mod_own, mod_all.at[source], mod_recv.at[source]).wait()
        pltpu.make_async_copy(step_own, step_all.at[source], step_recv.at[source]).wait()

    def wide(row):
        return jnp.concatenate([row] * copies, axis=1)

    def columns(rows, ones_row):
        pad = (lax.broadcasted_iota(jnp.int32, (LANES - ones_row, hidden), 0) == 0).astype(F32)
        return jnp.concatenate([rows, pad], axis=0).T.astype(BF16)

    def spread(cols, picked, ones_row):
        row = lax.broadcasted_iota(jnp.int32, (LANES, LANES), 0)
        picks = []
        for at in picked:
            picks.append(jnp.where((row == at) | (row == ones_row), 0.5, 0.0).astype(BF16))
            picks.append(jnp.where(row == at + local_steps, 0.5, 0.0).astype(BF16))
        both = jnp.dot(cols, jnp.concatenate(picks, axis=1), preferred_element_type=F32)
        parts = [both[:, k * LANES:(k + 1) * LANES] for k in range(2 * len(picked))]
        return parts[0::2], parts[1::2]

    def start_rows(sources):
        rows = jnp.concatenate([mod_all[source].astype(F32) for source in sources], axis=0)
        ones_row = rows.shape[0]
        picked = [2 * local_steps * k + i for k in range(len(sources)) for i in range(local_steps)]
        muls, adds = spread(columns(rows, ones_row), picked, ones_row)
        for k in range(len(picked)):
            at = sources[k // local_steps] * local_steps + k % local_steps
            mul_all[at] = muls[k]
            add_all[at] = adds[k]

    def start_tile(sources, k):
        source, i = sources[k // local_steps], k % local_steps
        at = source * local_steps + i
        half = pre_init[...] * wide(mul_all[at]) + wide(add_all[at])
        act_init[k] = gelu_of_half(half)
        drift = jnp.dot(w_out_buf[...], act_init[k].astype(BF16), preferred_element_type=F32)
        first_drift[at] = drift * wide(step_all[source, pl.ds(i, 1), :])

    needed = (n_steps - SWEEPS) // local_steps
    has_own = me < needed
    nearest = jnp.where(has_own, chip, 0)
    order = [nearest] + [jnp.where(k - 1 < nearest, k - 1, k) for k in range(1, needed // 2)]
    one = 2 * nearest + jnp.where(has_own, core, 0)
    other = 2 * nearest + jnp.where(has_own, 1 - core, 1)

    @pl.when(me == 0)
    def _():
        send_noise()

    @pl.when(one != me)
    def _():
        wait_mods(one)

    start_rows([one])
    for k in range(local_steps):
        start_tile([one], k)
    wait_mods(other)
    start_rows([other])
    for k in range(local_steps):
        start_tile([other], k)

    @pl.when(me == 1)
    def _():
        send_noise()

    for chip_at in order[1:-1]:
        pair = [2 * chip_at, 2 * chip_at + 1]
        for source in pair:
            wait_mods(source)
        start_rows(pair)
        for k in range(2 * local_steps):
            start_tile(pair, k)

    @pl.when(me >= 2)
    def _():
        send_noise()

    pair = [2 * order[-1], 2 * order[-1] + 1]
    for source in pair + list(range(needed, n_time)):
        @pl.when((source != me) & (source != one) & (source != other))
        def _(source=source):
            wait_mods(source)
    start_rows(pair)
    start_rows(range(needed, n_time))

    def activate(pre, at, dst, index):
        half = pre * wide(mul_all[at]) + wide(add_all[at])
        dst[index] = gelu_of_half(half)

    def first_product(parity, s, parts=1):
        size = hidden // parts
        latent = versions[parity, s].astype(BF16)
        return jnp.concatenate([jnp.dot(w_in_t[k * size:(k + 1) * size, :], latent, preferred_element_type=F32) for k in range(parts)], axis=0)

    def update(block, i, s, act, base=None):
        at = block * local_steps + i
        done = s == SWEEPS - 1 or base is not None
        drift = jnp.dot(w_out_buf[...], act.astype(BF16), preferred_element_type=F32)
        step = wide(step_all[block + i // local_steps, pl.ds(i % local_steps, 1), :])
        latent = versions[i % 2, s + 1 if base is None else base] + (drift * step + noise_all[at])
        versions[1 - i % 2, s + 1] = latent
        if done:
            out_stage[at + 1] = latent
            if isinstance(block, int):
                send_ready(block, i + 1)

    def run_block(block, static_block=None, late=(), last=False, filler=(), upward=False):
        filler = list(filler)
        block_parts = last or static_block == 0
        late_act = late_pre = None
        if late:
            late_act, late_pre = late

        def finish(tile):
            if tile == "late":
                update(*late_pre, act_late[...])
                return
            i, s = tile
            fresh = static_block is not None and s == static_block * local_steps + i
            update(block, i, s, act_buf[(i % 2) * SWEEPS + s], s if fresh else None)

        def ranges(i):
            if static_block is None:
                return 1, SWEEPS - 1, True
            j = static_block * local_steps + i
            low = SWEEPS - (n_steps - 1 - j)
            return max(1, low), min(j, SWEEPS - 1), low <= 0

        tiles = [(i, s) for i in range(local_steps) for s in range(ranges(i)[1], ranges(i)[0] - 1, -1)]
        if upward:
            tiles.sort()
        begun = {}

        def begin(tile):
            begun[tile] = first_product(tile[0] % 2, tile[1], 2 if block_parts else 1)

        pending = []
        for i in range(local_steps):
            low, high, needs_first = ranges(i)
            mine = [t for t in tiles if t[0] == i]
            if mine:
                begin(mine[0])
            if late_act is not None:
                update(*late_act, act_late[...])
                activate(pre_late[...], late_pre[0] * local_steps + late_pre[1], act_late, ...)
                pending.append("late")
                late_act = None
                if upward:
                    finish(pending.pop())
            for k, tile in enumerate(mine):
                if k + 1 < len(mine):
                    begin(mine[k + 1])
                pre = begun.pop(tile)
                if not last and tile == tiles[-1]:
                    pre_late[...] = pre
                    late_pre_out = (block, i, tile[1])
                    continue
                if not last and tile == tiles[-2]:
                    activate(pre, block * local_steps + i, act_late, ...)
                    late_act_out = (block, i, tile[1])
                else:
                    activate(pre, block * local_steps + i, act_buf, (i % 2) * SWEEPS + tile[1])
                    pending.append(tile)
                while len(pending) > 1:
                    finish(pending.pop(0))
                if filler:
                    filler.pop(0)()
            while pending:
                finish(pending.pop(0))
            if needs_first:
                at = block * local_steps + i
                fresh = static_block is not None and at == 0
                latent = versions[i % 2, 0 if fresh else 1] + (first_drift[at] + noise_all[at])
                versions[1 - i % 2, 1] = latent
                if fresh:
                    out_stage[1] = latent
        for work in filler:
            work()
        if not last:
            return late_act_out, late_pre_out

    def wait_noise(block):
        dst = noise_all.at[pl.ds(block * local_steps, local_steps)]
        pltpu.make_async_copy(noise_ref.at[:, me], dst, noise_recv.at[block]).wait()

    def send_steps(block, first, count):
        own = block == me
        send(out_stage.at[pl.ds(block * local_steps + first, count)],
             gathered.at[pl.ds(first, count), jnp.where(own, n_time, me)],
             out_send.at[block], out_recv.at[jnp.where(own, n_time, me)], jnp.where(own, partner, block))

    def send_ready(block, i):
        block, i = block + i // local_steps, i % local_steps
        if block == n_time - 2 and i >= local_steps - 2:
            if i == local_steps - 2:
                send_steps(block, 0, i + 1)
            else:
                send_steps(block, i, 1)
        if block == n_time - 1:
            send_steps(block, i, 1)

    full_from = -(-(SWEEPS - 1) // local_steps)
    full_to = (n_steps - SWEEPS) // local_steps

    late = ()
    for block in range(full_from):
        wait_noise(block)
        if block > 0:
            send_steps(block - 1, 0, local_steps)
        filler = [functools.partial(start_tile, pair, k) for k in range(2 * local_steps)] if block == 0 else ()
        late = run_block(block, block, late, filler=filler)

    def late_of(block):
        return (block, local_steps - 1, 2), (block, local_steps - 1, 1)

    def body(block, carry):
        wait_noise(block)
        send_steps(block - 1, 0, local_steps)
        run_block(block, None, late_of(block - 1))
        return carry

    lax.fori_loop(full_from, full_to, body, 0)
    late = late_of(full_to - 1)
    for block in range(full_to, n_time):
        wait_noise(block)
        if block == full_to:
            send_steps(block - 1, 0, local_steps)
        late = run_block(block, block, late, last=block == n_time - 1, upward=block >= UPWARD)

    for k in range(n_time - 1):
        noise_copy(k).wait_send()

    for copy in sends:
        copy.wait_send()
    for away in range(n_time):
        other = lax.rem(me + away, n_time)
        slot = n_time if away == 0 else other
        done = pltpu.make_async_remote_copy(src_ref=out_stage.at[pl.ds(other * local_steps, local_steps)], dst_ref=gathered.at[:, slot],
                                            send_sem=out_send.at[other], recv_sem=out_recv.at[slot],
                                            device_id={"time": partner}, device_id_type=MESH)
        done.wait_send()
        done.wait_recv()
        if away == 0:
            out_ref[:, me] = out_stage[pl.ds(me * local_steps, local_steps)]
        else:
            out_ref[:, other] = gathered[:, other]


def solution(mesh):
    n_time = mesh.shape["time"]

    def body(x_init, w_in, w_out, mod_scale, mod_shift, step_size, noise_inc):
        local_steps, batch, tokens, channels = noise_inc.shape
        hidden = w_in.shape[1]
        assert batch == n_time and n_time % 2 == 0
        x_t = jnp.swapaxes(x_init, 1, 2)
        noise_t = jnp.swapaxes(noise_inc, 2, 3)
        n_steps = n_time * local_steps
        vmem = pl.BlockSpec(memory_space=pltpu.VMEM)
        anywhere = pl.BlockSpec(memory_space=pl.ANY)
        dma = pltpu.SemaphoreType.DMA
        out = pl.pallas_call(
            functools.partial(sampler_kernel, n_time),
            out_shape=pltpu.VMEM(noise_t.shape, F32),
            in_specs=[anywhere] * 7,
            out_specs=vmem,
            scratch_shapes=[
                pltpu.VMEM((channels, tokens), F32),
                pltpu.VMEM((channels, hidden), BF16),
                pltpu.VMEM((channels, hidden), BF16),
                pltpu.VMEM((local_steps, hidden), BF16),
                pltpu.VMEM((local_steps, hidden), BF16),
                pltpu.SMEM((local_steps,), F32),
                pltpu.VMEM((local_steps, n_time, channels, tokens), F32),
                pltpu.VMEM((hidden, channels), BF16),
                pltpu.VMEM((2 * local_steps, hidden), BF16),
                pltpu.VMEM((2 * local_steps, LANES), F32),
                pltpu.VMEM((n_time, 2 * local_steps, hidden), BF16),
                pltpu.VMEM((n_time, 2 * local_steps, LANES), F32),
                pltpu.VMEM((n_steps, hidden, LANES), F32),
                pltpu.VMEM((n_steps, hidden, LANES), F32),
                pltpu.VMEM((hidden, tokens), F32),
                pltpu.VMEM((n_steps, channels, tokens), F32),
                pltpu.VMEM((2, SWEEPS + 1, channels, tokens), F32),
                pltpu.VMEM((2 * SWEEPS, hidden, tokens), F32),
                pltpu.VMEM((hidden, tokens), F32),
                pltpu.VMEM((hidden, tokens), F32),
                pltpu.VMEM((2 * local_steps, hidden, tokens), F32),
                pltpu.VMEM((n_steps, channels, tokens), F32),
                pltpu.VMEM((n_steps, channels, tokens), F32),
                pltpu.VMEM((local_steps, n_time + 1, channels, tokens), F32),
                dma((7,)), dma((n_time,)), dma((n_time,)), dma((n_time,)), dma((n_time,)),
                dma((n_time,)), dma((n_time,)), dma((n_time,)), dma((n_time + 1,)),
            ],
            compiler_params=pltpu.CompilerParams(collective_id=0, has_side_effects=True),
        )(x_t, w_in, w_out.T, mod_scale, mod_shift, step_size, noise_t)
        return jnp.swapaxes(out, 2, 3)

    return jax.shard_map(
        body,
        mesh=mesh,
        in_specs=(P("data"), P(), P(), P("time"), P("time"), P("time"), P("time", "data")),
        out_specs=P("time", "data"),
        check_vma=False,
    )
```

```python
import functools
import math

import jax
import jax.numpy as jnp
from jax import lax
from jax.experimental import pallas as pl
from jax.experimental.pallas import tpu as pltpu
from jax.sharding import PartitionSpec as P

SWEEPS = 8
LANES = 128
F32 = jnp.float32
BF16 = jnp.bfloat16
MESH = pl.DeviceIdType.MESH
GELU_1 = 2.0 * math.sqrt(2.0 / math.pi)
GELU_3 = 4.0 * 0.044715 * GELU_1


def gelu_of_half(half):
    inner = half * (half * half * GELU_3 + GELU_1)
    return half + half * jnp.tanh(inner)


def sampler_kernel(n_time, x_ref, w_in_ref, w_out_ref, scale_ref, shift_ref, step_ref, noise_ref, out_ref,
                   x_buf, w_in_buf, w_out_buf, scale_buf, shift_buf, step_buf, noise_buf,
                   w_in_t, mod_own, step_own, mod_all, step_all, mul_all, add_all, pre_init, first_drift,
                   versions, act_buf, act_late, pre_late, act_init, noise_all, out_stage, gathered,
                   load_sem, mod_send, mod_recv, step_send, step_recv, noise_send, noise_recv, out_send, out_recv):
    me = lax.axis_index("time")
    local_steps = scale_ref.shape[0]
    partner = me + 1 - 2 * lax.rem(me, 2)
    n_steps = n_time * local_steps
    hidden = w_in_ref.shape[1]
    tokens = x_buf.shape[1]
    copies = tokens // LANES

    barrier = pltpu.get_barrier_semaphore()
    for away in range(1, n_time):
        pl.semaphore_signal(barrier, inc=1, device_id={"time": lax.rem(me + away, n_time)}, device_id_type=MESH)

    loads = [
        pltpu.make_async_copy(src, dst, load_sem.at[k])
        for k, (src, dst) in enumerate([(scale_ref, scale_buf), (shift_ref, shift_buf), (step_ref, step_buf),
                                        (w_in_ref, w_in_buf), (x_ref.at[me], x_buf), (w_out_ref, w_out_buf)])
    ]
    for copy in loads:
        copy.start()
    own_noise = pltpu.make_async_copy(noise_ref.at[:, me], noise_all.at[pl.ds(me * local_steps, local_steps)], noise_recv.at[me])
    own_noise.start()
    noise_load = pltpu.make_async_copy(noise_ref, noise_buf, load_sem.at[len(loads)])
    noise_load.start()
    for copy in loads:
        copy.wait()
    mod_own[0:local_steps, :] = scale_buf[...]
    mod_own[local_steps:2 * local_steps, :] = shift_buf[...]
    for i in range(local_steps):
        step_own[i:i + 1, :] = jnp.full((1, LANES), step_buf[i], F32)
    mod_all[me] = mod_own[...]
    step_all[me] = step_own[...]
    w_in_t[...] = w_in_buf[...].astype(F32).T.astype(BF16)

    x0 = x_buf[...]
    versions[0, 0] = x0
    versions[1, 0] = x0
    out_stage[0] = x0
    pre_init[...] = jnp.dot(w_in_t[...], x0.astype(BF16), preferred_element_type=F32)

    pl.semaphore_wait(barrier, n_time - 1)

    sends = []

    def send(src, dst, send_sem, recv_sem, target):
        copy = pltpu.make_async_remote_copy(src_ref=src, dst_ref=dst, send_sem=send_sem, recv_sem=recv_sem,
                                            device_id={"time": target}, device_id_type=MESH)
        copy.start()
        return copy

    n_chips = n_time // 2
    chip, core = me // 2, lax.rem(me, 2)
    apart = sorted(range(1, n_chips), key=lambda hops: -min(hops, n_chips - hops))
    peers = [2 * lax.rem(chip + hops, n_chips) + c for hops in apart for c in range(2)] + [partner]
    for k, target in enumerate(peers):
        sends.append(send(mod_own, mod_all.at[me], mod_send.at[k], mod_recv.at[me], target))
        sends.append(send(step_own, step_all.at[me], step_send.at[k], step_recv.at[me], target))
    noise_load.wait()

    def noise_copy(k):
        return pltpu.make_async_remote_copy(
            src_ref=noise_buf.at[:, peers[k]], dst_ref=noise_all.at[pl.ds(me * local_steps, local_steps)],
            send_sem=noise_send.at[k], recv_sem=noise_recv.at[me], device_id={"time": peers[k]}, device_id_type=MESH)

    def send_noise():
        for k in range(n_time - 1):
            noise_copy(k).start()

    def wait_mods(source):
        pltpu.make_async_copy(mod_own, mod_all.at[source], mod_recv.at[source]).wait()
        pltpu.make_async_copy(step_own, step_all.at[source], step_recv.at[source]).wait()

    def wide(row):
        return jnp.concatenate([row] * copies, axis=1)

    def columns(rows, ones_row):
        pad = (lax.broadcasted_iota(jnp.int32, (LANES - ones_row, hidden), 0) == 0).astype(F32)
        return jnp.concatenate([rows, pad], axis=0).T.astype(BF16)

    def spread(cols, picked, ones_row):
        row = lax.broadcasted_iota(jnp.int32, (LANES, LANES), 0)
        picks = []
        for at in picked:
            picks.append(jnp.where((row == at) | (row == ones_row), 0.5, 0.0).astype(BF16))
            picks.append(jnp.where(row == at + local_steps, 0.5, 0.0).astype(BF16))
        both = jnp.dot(cols, jnp.concatenate(picks, axis=1), preferred_element_type=F32)
        parts = [both[:, k * LANES:(k + 1) * LANES] for k in range(2 * len(picked))]
        return parts[0::2], parts[1::2]

    def start_rows(sources):
        rows = jnp.concatenate([mod_all[source].astype(F32) for source in sources], axis=0)
        ones_row = rows.shape[0]
        picked = [2 * local_steps * k + i for k in range(len(sources)) for i in range(local_steps)]
        muls, adds = spread(columns(rows, ones_row), picked, ones_row)
        for k in range(len(picked)):
            at = sources[k // local_steps] * local_steps + k % local_steps
            mul_all[at] = muls[k]
            add_all[at] = adds[k]

    def start_tile(sources, k):
        source, i = sources[k // local_steps], k % local_steps
        at = source * local_steps + i
        half = pre_init[...] * wide(mul_all[at]) + wide(add_all[at])
        act_init[k] = gelu_of_half(half)
        drift = jnp.dot(w_out_buf[...], act_init[k].astype(BF16), preferred_element_type=F32)
        first_drift[at] = drift * wide(step_all[source, pl.ds(i, 1), :])

    needed = (n_steps - SWEEPS) // local_steps
    has_own = me < needed
    nearest = jnp.where(has_own, chip, 0)
    order = [nearest] + [jnp.where(k - 1 < nearest, k - 1, k) for k in range(1, needed // 2)]
    one = 2 * nearest + jnp.where(has_own, core, 0)
    other = 2 * nearest + jnp.where(has_own, 1 - core, 1)

    @pl.when(me == 0)
    def _():
        send_noise()

    @pl.when(one != me)
    def _():
        wait_mods(one)

    start_rows([one])
    for k in range(local_steps):
        start_tile([one], k)
    wait_mods(other)
    start_rows([other])
    for k in range(local_steps):
        start_tile([other], k)

    @pl.when((me >= 1) & (me < 4))
    def _():
        send_noise()

    for chip_at in order[1:-1]:
        pair = [2 * chip_at, 2 * chip_at + 1]
        for source in pair:
            wait_mods(source)
        start_rows(pair)
        for k in range(2 * local_steps):
            start_tile(pair, k)

    @pl.when(me >= 4)
    def _():
        send_noise()

    pair = [2 * order[-1], 2 * order[-1] + 1]
    for source in pair + list(range(needed, n_time)):
        @pl.when((source != me) & (source != one) & (source != other))
        def _(source=source):
            wait_mods(source)
    start_rows(pair)
    start_rows(range(needed, n_time))

    def activate(pre, at, dst, index):
        half = pre * wide(mul_all[at]) + wide(add_all[at])
        dst[index] = gelu_of_half(half)

    def first_product(parity, s):
        return jnp.dot(w_in_t[...], versions[parity, s].astype(BF16), preferred_element_type=F32)

    def update(block, i, s, act, base=None):
        at = block * local_steps + i
        done = s == SWEEPS - 1 or base is not None
        drift = jnp.dot(w_out_buf[...], act.astype(BF16), preferred_element_type=F32)
        step = wide(step_all[block + i // local_steps, pl.ds(i % local_steps, 1), :])
        latent = versions[i % 2, s + 1 if base is None else base] + (drift * step + noise_all[at])
        versions[1 - i % 2, s + 1] = latent
        if done:
            out_stage[at + 1] = latent
            if isinstance(block, int):
                send_ready(block, i + 1)

    def run_block(block, static_block=None, late=(), last=False, filler=()):
        filler = list(filler)
        late_act = late_pre = None
        if late:
            late_act, late_pre = late

        def finish(tile):
            if tile == "late":
                update(*late_pre, act_late[...])
                return
            i, s = tile
            fresh = static_block is not None and s == static_block * local_steps + i
            update(block, i, s, act_buf[(i % 2) * SWEEPS + s], s if fresh else None)

        def ranges(i):
            if static_block is None:
                return 1, SWEEPS - 1, True
            j = static_block * local_steps + i
            low = SWEEPS - (n_steps - 1 - j)
            return max(1, low), min(j, SWEEPS - 1), low <= 0

        tiles = [(i, s) for i in range(local_steps) for s in range(ranges(i)[1], ranges(i)[0] - 1, -1)]
        begun = {}

        def begin(tile):
            begun[tile] = first_product(tile[0] % 2, tile[1])

        pending = []
        for i in range(local_steps):
            low, high, needs_first = ranges(i)
            mine = [t for t in tiles if t[0] == i]
            if mine:
                begin(mine[0])
            if late_act is not None:
                update(*late_act, act_late[...])
                activate(pre_late[...], late_pre[0] * local_steps + late_pre[1], act_late, ...)
                pending.append("late")
                late_act = None
            for k, tile in enumerate(mine):
                if k + 1 < len(mine):
                    begin(mine[k + 1])
                pre = begun.pop(tile)
                if not last and tile == tiles[-1]:
                    pre_late[...] = pre
                    late_pre_out = (block, i, tile[1])
                    continue
                if not last and tile == tiles[-2]:
                    activate(pre, block * local_steps + i, act_late, ...)
                    late_act_out = (block, i, tile[1])
                else:
                    activate(pre, block * local_steps + i, act_buf, (i % 2) * SWEEPS + tile[1])
                    pending.append(tile)
                while len(pending) > 1:
                    finish(pending.pop(0))
                if filler:
                    filler.pop(0)()
            while pending:
                finish(pending.pop(0))
            if needs_first:
                at = block * local_steps + i
                fresh = static_block is not None and at == 0
                latent = versions[i % 2, 0 if fresh else 1] + (first_drift[at] + noise_all[at])
                versions[1 - i % 2, 1] = latent
                if fresh:
                    out_stage[1] = latent
        for work in filler:
            work()
        if not last:
            return late_act_out, late_pre_out

    def wait_noise(block):
        dst = noise_all.at[pl.ds(block * local_steps, local_steps)]
        pltpu.make_async_copy(noise_ref.at[:, me], dst, noise_recv.at[block]).wait()

    def send_steps(block, first, count):
        own = block == me
        send(out_stage.at[pl.ds(block * local_steps + first, count)],
             gathered.at[pl.ds(first, count), jnp.where(own, n_time, me)],
             out_send.at[block], out_recv.at[jnp.where(own, n_time, me)], jnp.where(own, partner, block))

    def send_ready(block, i):
        block, i = block + i // local_steps, i % local_steps
        if block == n_time - 2 and i >= local_steps - 2:
            if i == local_steps - 2:
                send_steps(block, 0, i + 1)
            else:
                send_steps(block, i, 1)
        if block == n_time - 1:
            send_steps(block, i, 1)

    full_from = -(-(SWEEPS - 1) // local_steps)
    full_to = (n_steps - SWEEPS) // local_steps

    late = ()
    for block in range(full_from):
        wait_noise(block)
        if block > 0:
            send_steps(block - 1, 0, local_steps)
        filler = [functools.partial(start_tile, pair, k) for k in range(2 * local_steps)] if block == 0 else ()
        late = run_block(block, block, late, filler=filler)

    def late_of(block):
        return (block, local_steps - 1, 2), (block, local_steps - 1, 1)

    def body(block, carry):
        wait_noise(block)
        send_steps(block - 1, 0, local_steps)
        run_block(block, None, late_of(block - 1))
        return carry

    lax.fori_loop(full_from, full_to, body, 0)
    late = late_of(full_to - 1)
    for block in range(full_to, n_time):
        wait_noise(block)
        if block == full_to:
            send_steps(block - 1, 0, local_steps)
        late = run_block(block, block, late, last=block == n_time - 1)

    for k in range(n_time - 1):
        noise_copy(k).wait_send()

    for copy in sends:
        copy.wait_send()
    for away in range(n_time):
        other = lax.rem(me + away, n_time)
        slot = n_time if away == 0 else other
        done = pltpu.make_async_remote_copy(src_ref=out_stage.at[pl.ds(other * local_steps, local_steps)], dst_ref=gathered.at[:, slot],
                                            send_sem=out_send.at[other], recv_sem=out_recv.at[slot],
                                            device_id={"time": partner}, device_id_type=MESH)
        done.wait_send()
        done.wait_recv()
        if away == 0:
            out_ref[:, me] = out_stage[pl.ds(me * local_steps, local_steps)]
        else:
            out_ref[:, other] = gathered[:, other]


def solution(mesh):
    n_time = mesh.shape["time"]

    def body(x_init, w_in, w_out, mod_scale, mod_shift, step_size, noise_inc):
        local_steps, batch, tokens, channels = noise_inc.shape
        hidden = w_in.shape[1]
        assert batch == n_time and n_time % 2 == 0
        x_t = jnp.swapaxes(x_init, 1, 2)
        noise_t = jnp.swapaxes(noise_inc, 2, 3)
        n_steps = n_time * local_steps
        vmem = pl.BlockSpec(memory_space=pltpu.VMEM)
        anywhere = pl.BlockSpec(memory_space=pl.ANY)
        dma = pltpu.SemaphoreType.DMA
        out = pl.pallas_call(
            functools.partial(sampler_kernel, n_time),
            out_shape=pltpu.VMEM(noise_t.shape, F32),
            in_specs=[anywhere] * 7,
            out_specs=vmem,
            scratch_shapes=[
                pltpu.VMEM((channels, tokens), F32),
                pltpu.VMEM((channels, hidden), BF16),
                pltpu.VMEM((channels, hidden), BF16),
                pltpu.VMEM((local_steps, hidden), BF16),
                pltpu.VMEM((local_steps, hidden), BF16),
                pltpu.SMEM((local_steps,), F32),
                pltpu.VMEM((local_steps, n_time, channels, tokens), F32),
                pltpu.VMEM((hidden, channels), BF16),
                pltpu.VMEM((2 * local_steps, hidden), BF16),
                pltpu.VMEM((2 * local_steps, LANES), F32),
                pltpu.VMEM((n_time, 2 * local_steps, hidden), BF16),
                pltpu.VMEM((n_time, 2 * local_steps, LANES), F32),
                pltpu.VMEM((n_steps, hidden, LANES), F32),
                pltpu.VMEM((n_steps, hidden, LANES), F32),
                pltpu.VMEM((hidden, tokens), F32),
                pltpu.VMEM((n_steps, channels, tokens), F32),
                pltpu.VMEM((2, SWEEPS + 1, channels, tokens), F32),
                pltpu.VMEM((2 * SWEEPS, hidden, tokens), F32),
                pltpu.VMEM((hidden, tokens), F32),
                pltpu.VMEM((hidden, tokens), F32),
                pltpu.VMEM((2 * local_steps, hidden, tokens), F32),
                pltpu.VMEM((n_steps, channels, tokens), F32),
                pltpu.VMEM((n_steps, channels, tokens), F32),
                pltpu.VMEM((local_steps, n_time + 1, channels, tokens), F32),
                dma((7,)), dma((n_time,)), dma((n_time,)), dma((n_time,)), dma((n_time,)),
                dma((n_time,)), dma((n_time,)), dma((n_time,)), dma((n_time + 1,)),
            ],
            compiler_params=pltpu.CompilerParams(collective_id=0, has_side_effects=True),
        )(x_t, w_in, w_out.T, mod_scale, mod_shift, step_size, noise_t)
        return jnp.swapaxes(out, 2, 3)

    return jax.shard_map(
        body,
        mesh=mesh,
        in_specs=(P("data"), P(), P(), P("time"), P("time"), P("time"), P("time", "data")),
        out_specs=P("time", "data"),
        check_vma=False,
    )
```

```python
import functools
import math

import jax
import jax.numpy as jnp
from jax import lax
from jax.experimental import pallas as pl
from jax.experimental.pallas import tpu as pltpu
from jax.sharding import PartitionSpec as P

SWEEPS = 8
LANES = 128
F32 = jnp.float32
BF16 = jnp.bfloat16
MESH = pl.DeviceIdType.MESH
GELU_1 = 2.0 * math.sqrt(2.0 / math.pi)
GELU_3 = 4.0 * 0.044715 * GELU_1


def gelu_of_half(half):
    inner = half * (half * half * GELU_3 + GELU_1)
    return half + half * jnp.tanh(inner)


def sampler_kernel(n_time, x_ref, w_in_ref, w_out_ref, scale_ref, shift_ref, step_ref, noise_ref, out_ref,
                   x_buf, w_in_buf, w_out_buf, scale_buf, shift_buf, step_buf, noise_buf,
                   w_in_t, mod_own, step_own, mod_all, step_all, mul_all, add_all, pre_init, first_drift,
                   versions, act_buf, act_late, pre_late, act_init, noise_all, out_stage, gathered,
                   load_sem, mod_send, mod_recv, step_send, step_recv, noise_send, noise_recv, out_send, out_recv):
    me = lax.axis_index("time")
    local_steps = scale_ref.shape[0]
    partner = me + 1 - 2 * lax.rem(me, 2)
    n_steps = n_time * local_steps
    hidden = w_in_ref.shape[1]
    tokens = x_buf.shape[1]
    copies = tokens // LANES

    barrier = pltpu.get_barrier_semaphore()
    for away in range(1, n_time):
        pl.semaphore_signal(barrier, inc=1, device_id={"time": lax.rem(me + away, n_time)}, device_id_type=MESH)

    loads = [
        pltpu.make_async_copy(src, dst, load_sem.at[k])
        for k, (src, dst) in enumerate([(scale_ref, scale_buf), (shift_ref, shift_buf), (step_ref, step_buf),
                                        (w_in_ref, w_in_buf), (x_ref.at[me], x_buf), (w_out_ref, w_out_buf)])
    ]
    for copy in loads:
        copy.start()
    half_steps = local_steps // 2
    for part in range(2):
        pltpu.make_async_copy(noise_ref.at[pl.ds(part * half_steps, half_steps), me],
                              noise_all.at[pl.ds(me * local_steps + part * half_steps, half_steps)], noise_recv.at[part, me]).start()
    noise_load = pltpu.make_async_copy(noise_ref, noise_buf, load_sem.at[len(loads)])
    noise_load.start()
    for copy in loads[:3]:
        copy.wait()
    mod_own[0:local_steps, :] = scale_buf[...]
    mod_own[local_steps:2 * local_steps, :] = shift_buf[...]
    for i in range(local_steps):
        step_own[i:i + 1, :] = jnp.full((1, LANES), step_buf[i], F32)
    mod_all[me] = mod_own[...]
    step_all[me] = step_own[...]
    pl.semaphore_wait(barrier, n_time - 1)

    sends = []

    def send(src, dst, send_sem, recv_sem, target):
        copy = pltpu.make_async_remote_copy(src_ref=src, dst_ref=dst, send_sem=send_sem, recv_sem=recv_sem,
                                            device_id={"time": target}, device_id_type=MESH)
        copy.start()
        return copy

    n_chips = n_time // 2
    chip, core = me // 2, lax.rem(me, 2)
    apart = sorted(range(1, n_chips), key=lambda hops: -min(hops, n_chips - hops))
    peers = [2 * lax.rem(chip + hops, n_chips) + c for hops in apart for c in range(2)] + [partner]
    for k, target in enumerate(peers):
        sends.append(send(mod_own, mod_all.at[me], mod_send.at[k], mod_recv.at[me], target))
        sends.append(send(step_own, step_all.at[me], step_send.at[k], step_recv.at[me], target))
    noise_load.wait()

    def noise_copy(part, k):
        return pltpu.make_async_remote_copy(
            src_ref=noise_buf.at[pl.ds(part * half_steps, half_steps), peers[k]],
            dst_ref=noise_all.at[pl.ds(me * local_steps + part * half_steps, half_steps)],
            send_sem=noise_send.at[part, k], recv_sem=noise_recv.at[part, me], device_id={"time": peers[k]}, device_id_type=MESH)

    def send_noise():
        for part in range(2):
            for k in range(n_time - 1):
                noise_copy(part, k).start()

    def wait_mods(source):
        pltpu.make_async_copy(mod_own, mod_all.at[source], mod_recv.at[source]).wait()
        pltpu.make_async_copy(step_own, step_all.at[source], step_recv.at[source]).wait()

    def wide(row):
        return jnp.concatenate([row] * copies, axis=1)

    def columns(rows, ones_row):
        pad = (lax.broadcasted_iota(jnp.int32, (LANES - ones_row, hidden), 0) == 0).astype(F32)
        return jnp.concatenate([rows, pad], axis=0).T.astype(BF16)

    def spread(cols, picked, ones_row):
        row = lax.broadcasted_iota(jnp.int32, (LANES, LANES), 0)
        picks = []
        for at in picked:
            picks.append(jnp.where((row == at) | (row == ones_row), 0.5, 0.0).astype(BF16))
            picks.append(jnp.where(row == at + local_steps, 0.5, 0.0).astype(BF16))
        both = jnp.dot(cols, jnp.concatenate(picks, axis=1), preferred_element_type=F32)
        parts = [both[:, k * LANES:(k + 1) * LANES] for k in range(2 * len(picked))]
        return parts[0::2], parts[1::2]

    def start_rows(sources):
        rows = jnp.concatenate([mod_all[source].astype(F32) for source in sources], axis=0)
        ones_row = rows.shape[0]
        picked = [2 * local_steps * k + i for k in range(len(sources)) for i in range(local_steps)]
        muls, adds = spread(columns(rows, ones_row), picked, ones_row)
        for k in range(len(picked)):
            at = sources[k // local_steps] * local_steps + k % local_steps
            mul_all[at] = muls[k]
            add_all[at] = adds[k]

    def start_tile(sources, k):
        source, i = sources[k // local_steps], k % local_steps
        at = source * local_steps + i
        half = pre_init[...] * wide(mul_all[at]) + wide(add_all[at])
        act_init[k] = gelu_of_half(half)
        drift = jnp.dot(w_out_buf[...], act_init[k].astype(BF16), preferred_element_type=F32)
        first_drift[at] = drift * wide(step_all[source, pl.ds(i, 1), :])

    needed = (n_steps - SWEEPS) // local_steps
    has_own = me < needed
    nearest = jnp.where(has_own, chip, 0)
    order = [nearest] + [jnp.where(k - 1 < nearest, k - 1, k) for k in range(1, needed // 2)]
    one = 2 * nearest + jnp.where(has_own, core, 0)
    other = 2 * nearest + jnp.where(has_own, 1 - core, 1)

    @pl.when(me == 0)
    def _():
        send_noise()

    for copy in loads[3:]:
        copy.wait()
    w_in_t[...] = w_in_buf[...].astype(F32).T.astype(BF16)

    x0 = x_buf[...]
    versions[0, 0] = x0
    versions[1, 0] = x0
    out_stage[0] = x0
    pre_init[...] = jnp.dot(w_in_t[...], x0.astype(BF16), preferred_element_type=F32)

    @pl.when(one != me)
    def _():
        wait_mods(one)

    start_rows([one])
    for k in range(local_steps):
        start_tile([one], k)
    wait_mods(other)
    start_rows([other])
    for k in range(local_steps):
        start_tile([other], k)

    @pl.when((me >= 1) & (me < 4))
    def _():
        send_noise()

    for chip_at in order[1:-1]:
        pair = [2 * chip_at, 2 * chip_at + 1]
        for source in pair:
            wait_mods(source)
        start_rows(pair)
        for k in range(2 * local_steps):
            start_tile(pair, k)

    @pl.when(me >= 4)
    def _():
        send_noise()

    pair = [2 * order[-1], 2 * order[-1] + 1]
    for source in pair + list(range(needed, n_time)):
        @pl.when((source != me) & (source != one) & (source != other))
        def _(source=source):
            wait_mods(source)
    start_rows(pair)
    start_rows(range(needed, n_time))

    def activate(pre, at, dst, index):
        half = pre * wide(mul_all[at]) + wide(add_all[at])
        dst[index] = gelu_of_half(half)

    def first_product(parity, s):
        return jnp.dot(w_in_t[...], versions[parity, s].astype(BF16), preferred_element_type=F32)

    def update(block, i, s, act, base=None):
        at = block * local_steps + i
        done = s == SWEEPS - 1 or base is not None
        drift = jnp.dot(w_out_buf[...], act.astype(BF16), preferred_element_type=F32)
        step = wide(step_all[block + i // local_steps, pl.ds(i % local_steps, 1), :])
        latent = versions[i % 2, s + 1 if base is None else base] + (drift * step + noise_all[at])
        versions[1 - i % 2, s + 1] = latent
        if done:
            out_stage[at + 1] = latent
            if isinstance(block, int):
                send_ready(block, i + 1)

    def run_block(block, static_block=None, late=(), last=False, filler=()):
        filler = list(filler)
        late_act = late_pre = None
        if late:
            late_act, late_pre = late

        def finish(tile):
            if tile == "late":
                update(*late_pre, act_late[...])
                return
            i, s = tile
            fresh = static_block is not None and s == static_block * local_steps + i
            update(block, i, s, act_buf[(i % 2) * SWEEPS + s], s if fresh else None)

        def ranges(i):
            if static_block is None:
                return 1, SWEEPS - 1, True
            j = static_block * local_steps + i
            low = SWEEPS - (n_steps - 1 - j)
            return max(1, low), min(j, SWEEPS - 1), low <= 0

        tiles = [(i, s) for i in range(local_steps) for s in range(ranges(i)[1], ranges(i)[0] - 1, -1)]
        begun = {}

        def begin(tile):
            begun[tile] = first_product(tile[0] % 2, tile[1])

        pending = []
        for i in range(local_steps):
            low, high, needs_first = ranges(i)
            if static_block == 0 and i == half_steps:
                wait_noise(block, (1,))
            mine = [t for t in tiles if t[0] == i]
            if mine:
                begin(mine[0])
            if late_act is not None:
                update(*late_act, act_late[...])
                activate(pre_late[...], late_pre[0] * local_steps + late_pre[1], act_late, ...)
                pending.append("late")
                late_act = None
            for k, tile in enumerate(mine):
                if k + 1 < len(mine):
                    begin(mine[k + 1])
                pre = begun.pop(tile)
                if not last and tile == tiles[-1]:
                    pre_late[...] = pre
                    late_pre_out = (block, i, tile[1])
                    continue
                if not last and tile == tiles[-2]:
                    activate(pre, block * local_steps + i, act_late, ...)
                    late_act_out = (block, i, tile[1])
                else:
                    activate(pre, block * local_steps + i, act_buf, (i % 2) * SWEEPS + tile[1])
                    pending.append(tile)
                while len(pending) > 1:
                    finish(pending.pop(0))
                if filler:
                    filler.pop(0)()
            while pending:
                finish(pending.pop(0))
            if needs_first:
                at = block * local_steps + i
                fresh = static_block is not None and at == 0
                latent = versions[i % 2, 0 if fresh else 1] + (first_drift[at] + noise_all[at])
                versions[1 - i % 2, 1] = latent
                if fresh:
                    out_stage[1] = latent
        for work in filler:
            work()
        if not last:
            return late_act_out, late_pre_out

    def wait_noise(block, parts=(0, 1)):
        for part in parts:
            pltpu.make_async_copy(noise_ref.at[pl.ds(part * half_steps, half_steps), me],
                                  noise_all.at[pl.ds(block * local_steps + part * half_steps, half_steps)],
                                  noise_recv.at[part, block]).wait()

    def send_steps(block, first, count):
        own = block == me
        send(out_stage.at[pl.ds(block * local_steps + first, count)],
             gathered.at[pl.ds(first, count), jnp.where(own, n_time, me)],
             out_send.at[block], out_recv.at[jnp.where(own, n_time, me)], jnp.where(own, partner, block))

    def send_ready(block, i):
        block, i = block + i // local_steps, i % local_steps
        if block == n_time - 2 and i >= local_steps - 2:
            if i == local_steps - 2:
                send_steps(block, 0, i + 1)
            else:
                send_steps(block, i, 1)
        if block == n_time - 1:
            send_steps(block, i, 1)

    full_from = -(-(SWEEPS - 1) // local_steps)
    full_to = (n_steps - SWEEPS) // local_steps

    late = ()
    for block in range(full_from):
        wait_noise(block, (0, 1) if block else (0,))
        if block > 0:
            send_steps(block - 1, 0, local_steps)
        filler = [functools.partial(start_tile, pair, k) for k in range(2 * local_steps)] if block == 0 else ()
        late = run_block(block, block, late, filler=filler)

    def late_of(block):
        return (block, local_steps - 1, 2), (block, local_steps - 1, 1)

    def body(block, carry):
        wait_noise(block)
        send_steps(block - 1, 0, local_steps)
        run_block(block, None, late_of(block - 1))
        return carry

    lax.fori_loop(full_from, full_to, body, 0)
    late = late_of(full_to - 1)
    for block in range(full_to, n_time):
        wait_noise(block)
        if block == full_to:
            send_steps(block - 1, 0, local_steps)
        late = run_block(block, block, late, last=block == n_time - 1)

    for part in range(2):
        for k in range(n_time - 1):
            noise_copy(part, k).wait_send()

    for copy in sends:
        copy.wait_send()
    for away in range(n_time):
        other = lax.rem(me + away, n_time)
        slot = n_time if away == 0 else other
        done = pltpu.make_async_remote_copy(src_ref=out_stage.at[pl.ds(other * local_steps, local_steps)], dst_ref=gathered.at[:, slot],
                                            send_sem=out_send.at[other], recv_sem=out_recv.at[slot],
                                            device_id={"time": partner}, device_id_type=MESH)
        done.wait_send()
        done.wait_recv()
        if away == 0:
            out_ref[:, me] = out_stage[pl.ds(me * local_steps, local_steps)]
        else:
            out_ref[:, other] = gathered[:, other]


def solution(mesh):
    n_time = mesh.shape["time"]

    def body(x_init, w_in, w_out, mod_scale, mod_shift, step_size, noise_inc):
        local_steps, batch, tokens, channels = noise_inc.shape
        hidden = w_in.shape[1]
        assert batch == n_time and n_time % 2 == 0
        x_t = jnp.swapaxes(x_init, 1, 2)
        noise_t = jnp.swapaxes(noise_inc, 2, 3)
        n_steps = n_time * local_steps
        vmem = pl.BlockSpec(memory_space=pltpu.VMEM)
        anywhere = pl.BlockSpec(memory_space=pl.ANY)
        dma = pltpu.SemaphoreType.DMA
        out = pl.pallas_call(
            functools.partial(sampler_kernel, n_time),
            out_shape=pltpu.VMEM(noise_t.shape, F32),
            in_specs=[anywhere] * 7,
            out_specs=vmem,
            scratch_shapes=[
                pltpu.VMEM((channels, tokens), F32),
                pltpu.VMEM((channels, hidden), BF16),
                pltpu.VMEM((channels, hidden), BF16),
                pltpu.VMEM((local_steps, hidden), BF16),
                pltpu.VMEM((local_steps, hidden), BF16),
                pltpu.SMEM((local_steps,), F32),
                pltpu.VMEM((local_steps, n_time, channels, tokens), F32),
                pltpu.VMEM((hidden, channels), BF16),
                pltpu.VMEM((2 * local_steps, hidden), BF16),
                pltpu.VMEM((2 * local_steps, LANES), F32),
                pltpu.VMEM((n_time, 2 * local_steps, hidden), BF16),
                pltpu.VMEM((n_time, 2 * local_steps, LANES), F32),
                pltpu.VMEM((n_steps, hidden, LANES), F32),
                pltpu.VMEM((n_steps, hidden, LANES), F32),
                pltpu.VMEM((hidden, tokens), F32),
                pltpu.VMEM((n_steps, channels, tokens), F32),
                pltpu.VMEM((2, SWEEPS + 1, channels, tokens), F32),
                pltpu.VMEM((2 * SWEEPS, hidden, tokens), F32),
                pltpu.VMEM((hidden, tokens), F32),
                pltpu.VMEM((hidden, tokens), F32),
                pltpu.VMEM((2 * local_steps, hidden, tokens), F32),
                pltpu.VMEM((n_steps, channels, tokens), F32),
                pltpu.VMEM((n_steps, channels, tokens), F32),
                pltpu.VMEM((local_steps, n_time + 1, channels, tokens), F32),
                dma((7,)), dma((n_time,)), dma((n_time,)), dma((n_time,)), dma((n_time,)),
                dma((2, n_time)), dma((2, n_time)), dma((n_time,)), dma((n_time + 1,)),
            ],
            compiler_params=pltpu.CompilerParams(collective_id=0, has_side_effects=True),
        )(x_t, w_in, w_out.T, mod_scale, mod_shift, step_size, noise_t)
        return jnp.swapaxes(out, 2, 3)

    return jax.shard_map(
        body,
        mesh=mesh,
        in_specs=(P("data"), P(), P(), P("time"), P("time"), P("time"), P("time", "data")),
        out_specs=P("time", "data"),
        check_vma=False,
    )
```
